32 devices in a mesh: dp: 8 (over y, x, core), tensor: 4 (over z).
Axes of the slice: x: 2, y: 2, z: 4, core: 2. Of those that a mesh axis runs over, the one named last changes fastest.
Arguments:
- tokens: bfloat16 [128, 8192], P('dp'), may hold values from -6 to 6
- norm_gain: bfloat16 [8192], replicated, may hold values from 0.099609375 to 1.8984375
- w_query: bfloat16 [8192, 8192], P('dp', 'tensor'), may hold values from -0.0625 to 0.0625
- w_key: bfloat16 [8192, 1024], P('dp', 'tensor'), may hold values from -0.0625 to 0.0625
- w_value: bfloat16 [8192, 1024], P('dp', 'tensor'), may hold values from -0.0625 to 0.0625
- check_column: bfloat16 [8192], replicated, may hold values from -6 to 6
- key_cache: bfloat16 [4096, 16, 8, 128], P('dp', None, 'tensor'), may hold values from -320 to 320
- value_cache: bfloat16 [4096, 16, 8, 128], P('dp', None, 'tensor'), may hold values from -6 to 6
- page_table: int32 [128, 32], P('dp'), may hold values from 0 to 511, as said below
- lengths: int32 [128], P('dp'), may hold values from 1 to 512, as said below
- tol_counts: int32 [128], replicated, may hold values from 0 to 7
Outputs:
- attention: bfloat16 [128, 8192], P('dp', 'tensor')
- excess: float32 [], replicated
The draws below stay inside these ranges and needn't reach their ends.
Inputs may be any that keep to these rules, and one draw needn't show every extreme that they name: page_table holds pool pages of the index of dp that holds the sequence; the 16 sequences of one index of dp own distinct pages and together own all 512 of them. `lengths`: some sequence holds exactly 512 cached tokens.
All inputs are finite; a program needn't handle non-finite values.
Results may differ from the reference program's by a relative error of at most 0.007.
The reference program's roundings to bfloat16 on the way count: a program that leaves them out, or rounds other values in their place, can miss the bound.
Values may be sent and summed in bfloat16 or wider, within the bound.
A program may use at most 64 MiB of HBM per device.

```python
import jax
import jax.numpy as jnp
from jax import lax

D = 8192
HQ = 64
KVH = 8
HD = 128
SEQ_DEV = 16
MAXP = 32
PAGE = 16
CTX = 512
POOL = 512
PAGES_ALL = 4096
B = 128


def draw_page_table(key, part):
    subkeys = jax.random.split(key, B // SEQ_DEV)

    def one_order(subkey):
        return jax.random.permutation(subkey, SEQ_DEV * MAXP)
    orders = jax.vmap(one_order)(subkeys)
    return orders.reshape(B, MAXP).astype(jnp.int32)


def draw_lengths(key, part):
    drawn = jax.random.randint(jax.random.fold_in(key, 3), (B,), 1, CTX + 1)
    return drawn.at[0].set(CTX).astype(jnp.int32)


def draw_key_cache(key, part):
    normal_part = jax.random.truncated_normal(jax.random.fold_in(key, 5), -4.0, 4.0, (PAGES_ALL, PAGE, KVH, HD), jnp.float32)
    return (normal_part * 2.2).astype(jnp.bfloat16)


def set_ends(result, own_key, low, high):
    longest = result.shape.index(max(result.shape))
    spots = []
    for shift in (0, 1):
        where = [jax.random.randint(jax.random.fold_in(own_key, axis), (), 0, length) for axis, length in enumerate(result.shape)]
        where[longest] = (where[longest] + shift) % result.shape[longest]
        spots.append(tuple(where))
    return result.at[spots[0]].set(low).at[spots[1]].set(high)


def block_scale(rng, shape, cuts, smallest, top_value):
    def one(position, blocks):
        steps = jax.random.uniform(jax.random.fold_in(jax.random.fold_in(rng, 6), position), (blocks,), jnp.float32, smallest / len(cuts), top_value / len(cuts))
        return jnp.repeat(jnp.exp(steps), shape[position] // blocks).reshape((-1,) + (1,) * (len(shape) - position - 1))

    loudness = one(*cuts[0])
    for cut in cuts[1:]:
        loudness = loudness * one(*cut)
    return loudness


def gaussian(rng, extent, spread, most, cuts=(), kind=jnp.bfloat16):
    result = jax.random.normal(rng, extent, jnp.float32) * spread
    if len(cuts) > 0:
        result = block_scale(rng, extent, cuts, -0.22, 0.18) * result
    return jnp.clip(result, min=-most, max=most).astype(kind)


def setup_inputs(seed: int = 0) -> dict:
    splits = jax.random.split(jax.random.key(seed), 12)
    tokens = gaussian(splits[0], (B, D), 1.0, 6.0, ((0, 8),))
    norm_gain = jnp.clip(1.0 + 0.18 * jax.random.normal(splits[1], (D,), jnp.float32), 0.099609375, 1.8984375).astype(jnp.bfloat16)
    w_query = gaussian(splits[2], (D, HQ * HD), D ** -0.5, 0.0625, ((0, 8), (1, 4)))
    w_key = gaussian(splits[3], (D, KVH * HD), D ** -0.5, 0.0625, ((0, 8), (1, 4)))
    w_value = gaussian(splits[4], (D, KVH * HD), D ** -0.5, 0.0625, ((0, 8), (1, 4)))
    check_column = gaussian(splits[5], (D,), (((HQ + 2 * KVH) * HD / D) ** 0.5), 6.0)
    key_cache = draw_key_cache(jax.random.fold_in(splits[11], 71), 0)
    value_cache = gaussian(splits[7], (PAGES_ALL, PAGE, KVH, HD), 1.0, 6.0, ((0, 8), (2, 4)))
    page_table = draw_page_table(jax.random.fold_in(splits[11], 71), 0)
    lengths = draw_lengths(jax.random.fold_in(splits[11], 71), 0)
    tol_counts = set_ends(jax.random.randint(splits[10], (B,), 0, 8), jax.random.fold_in(splits[10], 1), 0, 7).astype(jnp.int32)
    return {"tokens": tokens, "norm_gain": norm_gain, "w_query": w_query, "w_key": w_key, "w_value": w_value, "check_column": check_column, "key_cache": key_cache, "value_cache": value_cache, "page_table": page_table, "lengths": lengths, "tol_counts": tol_counts}


epsilon = 1e-06
rope_base = 1000000.0
tol_step = 0.25

def normalize(tokens, norm_gain):
    widened = tokens.astype(jnp.float32)
    mean_square = lax.optimization_barrier(jnp.mean(widened * widened, axis=1, keepdims=True))
    return (widened * lax.rsqrt(mean_square + epsilon) * norm_gain.astype(jnp.float32)).astype(jnp.bfloat16)

def rotate(vectors, positions):
    half_width = vectors.shape[-1] // 2
    steps_index = jnp.arange(half_width, dtype=jnp.float32)
    inverse = rope_base ** (-2.0 * steps_index / vectors.shape[-1])
    angles = positions.astype(jnp.float32)[:, None] * inverse[None, :]
    cosine = jnp.cos(angles)[:, None, :]
    sine_part = jnp.sin(angles)[:, None, :]
    lower = vectors[..., :half_width]
    upper = vectors[..., half_width:]
    return jnp.concatenate([lower * cosine - upper * sine_part, upper * cosine + lower * sine_part], axis=-1)

def attend(query_heads, cached_keys, cached_values, key_new, value_new, lengths):
    score_scale = query_heads.shape[-1] ** (-0.5)
    query_wide = query_heads.astype(jnp.float32)
    scores = jnp.einsum('skgd,sckd->skgc', query_wide, cached_keys.astype(jnp.float32)) * score_scale
    new_score = jnp.einsum('skgd,skd->skg', query_wide, key_new.astype(jnp.float32)) * score_scale
    live_mask = (jnp.arange(cached_keys.shape[1])[None, :] < lengths[:, None])[:, None, None, :]
    masked = jnp.where(live_mask, scores, -jnp.inf)
    peak_score = jnp.maximum(lax.optimization_barrier(jnp.max(masked, axis=-1)), new_score)
    weights = jnp.exp(masked - peak_score[..., None])
    new_weight = jnp.exp(new_score - peak_score)
    denominator = lax.optimization_barrier(jnp.sum(weights, axis=-1)) + new_weight
    rounded = lax.optimization_barrier(weights.astype(jnp.bfloat16)).astype(jnp.float32)
    rounded_new = lax.optimization_barrier(new_weight.astype(jnp.bfloat16)).astype(jnp.float32)
    mixed_heads = jnp.einsum('skgc,sckd->skgd', rounded, cached_values.astype(jnp.float32))
    mixed_heads = mixed_heads + rounded_new[..., None] * value_new.astype(jnp.float32)[:, :, None, :]
    return mixed_heads / denominator[..., None]

def reference(tokens, norm_gain, w_query, w_key, w_value, check_column, key_cache, value_cache, page_table, lengths, tol_counts):
    normed = normalize(tokens, norm_gain)
    query_all = jnp.dot(normed, w_query, preferred_element_type=jnp.float32)
    key_all = jnp.dot(normed, w_key, preferred_element_type=jnp.float32)
    value_all = jnp.dot(normed, w_value, preferred_element_type=jnp.float32)
    column_count = query_all.shape[1] + key_all.shape[1] + value_all.shape[1]
    row_sums = lax.optimization_barrier(jnp.sum(query_all, axis=1)) + lax.optimization_barrier(jnp.sum(key_all, axis=1)) + lax.optimization_barrier(jnp.sum(value_all, axis=1))
    check_sums = jnp.dot(normed, check_column, preferred_element_type=jnp.float32)
    residual = (row_sums - check_sums) / jnp.sqrt(jnp.float32(column_count))
    token_excess = jnp.maximum(jnp.abs(residual) - tol_step * tol_counts.astype(jnp.float32), 0.0)
    excess = jnp.sum(token_excess) / jnp.sqrt(jnp.float32(B))
    query_heads = rotate(query_all.reshape(B, HQ, HD), lengths).astype(jnp.bfloat16)
    key_new = rotate(key_all.reshape(B, KVH, HD), lengths).astype(jnp.bfloat16)
    value_new = value_all.reshape(B, KVH, HD).astype(jnp.bfloat16)
    owner_base = (jnp.arange(B) // SEQ_DEV * POOL).astype(jnp.int32)
    global_pages = (page_table + owner_base[:, None]).astype(jnp.int32)

    def one_sequence(inputs):
        query_one, key_one, value_one, pages_one, length_one = inputs
        cached_keys = key_cache[pages_one].reshape(1, CTX, KVH, HD)
        cached_values = value_cache[pages_one].reshape(1, CTX, KVH, HD)
        mixed_heads = attend(query_one.reshape(1, KVH, HQ // KVH, HD), cached_keys, cached_values, key_one[None], value_one[None], length_one[None])
        return mixed_heads.reshape(HQ * HD).astype(jnp.bfloat16)
    attention = lax.map(one_sequence, (query_heads, key_new, value_new, global_pages, lengths))
    return (attention, excess)
```

```python
import functools
import math

import jax
import jax.numpy as jnp
from jax import lax
from jax.experimental import pallas as pl
from jax.experimental.pallas import tpu as pltpu
from jax.sharding import PartitionSpec as P

EPSILON = 1e-06
ROPE_BASE = 1000000.0
TOL_STEP = 0.25
MESH = pl.DeviceIdType.MESH
F32 = jnp.float32
BF16 = jnp.bfloat16
UNROLL = 4


def step_kernel(
    dp,
    tp,
    table_ref,
    lengths_ref,
    counts_ref,
    tokens_ref,
    gain_ref,
    check_ref,
    cos_ref,
    sin_ref,
    wq_hbm,
    wk_hbm,
    wv_hbm,
    keys_hbm,
    values_hbm,
    out_ref,
    excess_ref,
    weights,
    keys,
    values,
    outgoing,
    spread,
    parts,
    from_pair,
    from_chips,
    queries,
    new_keys,
    new_values,
    mixed,
    sums_all,
    sums_own,
    excess_all,
    excess_own,
    load_sems,
    a2a_send,
    a2a_recv,
    pair_send,
    pair_recv,
    chip_send,
    chip_recv,
    sum_send,
    sum_recv,
    exc_send,
    exc_recv,
):
    chips = dp // 2
    me = lax.axis_index("dp")
    zed = lax.axis_index("tensor")
    chip, core = me // 2, me % 2
    seqs, width = tokens_ref.shape
    depth = width // dp
    q_width, kv_width = wq_hbm.shape[1], wk_hbm.shape[1]
    total = q_width + 2 * kv_width
    chunks, _, _, chunk = parts.shape
    head = keys_hbm.shape[2]
    q_heads, kv_heads = q_width // head, kv_width // head
    group = q_heads // kv_heads
    pages = table_ref.shape[1]
    page_rows = keys_hbm.shape[1]

    barrier = pltpu.get_barrier_semaphore()
    for k in range(1, dp):
        pl.semaphore_signal(
            barrier, inc=1, device_id=((me + k) % dp, zed), device_id_type=MESH
        )
    for k in range(1, tp):
        pl.semaphore_signal(
            barrier, inc=1, device_id=(me, (zed + k) % tp), device_id_type=MESH
        )

    loads = [
        pltpu.make_async_copy(wq_hbm, weights.at[:, pl.ds(0, q_width)], load_sems.at[0]),
        pltpu.make_async_copy(wk_hbm, weights.at[:, pl.ds(q_width, kv_width)], load_sems.at[1]),
        pltpu.make_async_copy(
            wv_hbm, weights.at[:, pl.ds(q_width + kv_width, kv_width)], load_sems.at[2]
        ),
        pltpu.make_async_copy(keys_hbm, keys, load_sems.at[3]),
        pltpu.make_async_copy(values_hbm, values, load_sems.at[4]),
    ]
    for load in loads:
        load.start()

    square = jnp.zeros((seqs, 1), F32)
    for j in range(dp):
        cols = pl.ds(j * depth, depth)
        part = tokens_ref[:, cols].astype(F32)
        square = square + jnp.sum(part * part, axis=1, keepdims=True)
    scale = lax.rsqrt(square / width + EPSILON)
    for j in range(dp):
        cols = pl.ds(j * depth, depth)
        outgoing[j] = (
            tokens_ref[:, cols].astype(F32) * scale * gain_ref[:, cols].astype(F32)
        ).astype(BF16)
    spread[0, 0] = outgoing[me]

    pl.semaphore_wait(barrier, dp - 1 + tp - 1)

    a2a = []
    for dc in range(chips - 1, -1, -1):
        for q in range(2):
            if dc == 0 and q == 0:
                continue
            target = ((chip + dc) % chips) * 2 + (core + q) % 2
            copy = pltpu.make_async_remote_copy(
                src_ref=outgoing.at[target],
                dst_ref=spread.at[q, dc],
                send_sem=a2a_send.at[q, dc],
                recv_sem=a2a_recv.at[q, dc],
                device_id=(target, zed),
                device_id_type=MESH,
            )
            copy.start()
            a2a.append(copy)

    check_sum = jnp.zeros((seqs, 1), F32)
    for j in range(dp):
        cols = pl.ds(j * depth, depth)
        check_sum = check_sum + jnp.sum(
            outgoing[j].astype(F32) * check_ref[:, cols].astype(F32), axis=1, keepdims=True
        )

    for load in loads[:3]:
        load.wait()
    for copy in a2a:
        copy.wait_recv()

    pair_copies, chip_copies = [], []
    half = chips * seqs

    def project(c):
        product = jnp.dot(
            spread[...].reshape(dp * seqs, depth),
            weights[:, pl.ds(c * chunk, chunk)],
            preferred_element_type=F32,
        )
        parts[c, 1] = product[half:]
        copy = pltpu.make_async_remote_copy(
            src_ref=parts.at[c, 1],
            dst_ref=from_pair.at[c],
            send_sem=pair_send.at[c],
            recv_sem=pair_recv.at[c],
            device_id=(chip * 2 + (core + 1) % 2, zed),
            device_id_type=MESH,
        )
        copy.start()
        pair_copies.append(copy)
        parts[c, 0] = product[:half]

    def pass_on(c):
        pair_copies[c].wait_recv()
        for dc in range(chips - 1, 0, -1):
            rows = pl.ds(dc * seqs, seqs)
            parts[c, 0, rows] = parts[c, 0, rows] + from_pair[c, rows]
            copy = pltpu.make_async_remote_copy(
                src_ref=parts.at[c, 0, rows],
                dst_ref=from_chips.at[c, dc - 1],
                send_sem=chip_send.at[c, dc - 1],
                recv_sem=chip_recv.at[c, dc - 1],
                device_id=(((chip + chips - dc) % chips) * 2 + core, zed),
                device_id_type=MESH,
            )
            copy.start()
            chip_copies.append(copy)

    for c in range(chunks):
        project(c)
        if c >= 1:
            pass_on(c - 1)
    pass_on(chunks - 1)

    def rotate(vector):
        return (
            (vector * cos_ref[...] + pltpu.roll(vector, head // 2, 1) * sin_ref[...])
            .astype(BF16)
            .astype(F32)
        )

    local_sum = jnp.zeros((seqs, 1), F32)
    for c in range(chunks):
        for copy in chip_copies[c * (chips - 1) : (c + 1) * (chips - 1)]:
            copy.wait_recv()
        own = parts[c, 0, pl.ds(0, seqs)] + from_pair[c, pl.ds(0, seqs)]
        for dc in range(1, chips):
            own = own + from_chips[c, dc - 1]
        local_sum = local_sum + jnp.sum(own, axis=1, keepdims=True)
        for i in range(chunk // head):
            block = own[:, i * head : (i + 1) * head]
            index = c * (chunk // head) + i
            if index < q_heads:
                queries[:, index, :] = rotate(block)
            elif index < q_heads + kv_heads:
                k = index - q_heads
                turned = rotate(block)
                for g in range(group):
                    new_keys[:, k * group + g, :] = turned
            else:
                k = index - q_heads - kv_heads
                rounded = block.astype(BF16).astype(F32)
                for g in range(group):
                    new_values[:, k * group + g, :] = rounded

    sums_own[...] = jnp.broadcast_to(local_sum, sums_own.shape)
    sums_all[zed] = sums_own[...]
    sum_copies = []
    for k in range(1, tp):
        copy = pltpu.make_async_remote_copy(
            src_ref=sums_own,
            dst_ref=sums_all.at[zed],
            send_sem=sum_send.at[k],
            recv_sem=sum_recv.at[k],
            device_id=(me, (zed + k) % tp),
            device_id_type=MESH,
        )
        copy.start()
        sum_copies.append(copy)

    span = pages * page_rows
    column = lax.broadcasted_iota(jnp.int32, (q_heads, span), 1)
    row = lax.broadcasted_iota(jnp.int32, (q_heads, span), 0)
    place = jnp.where(column % kv_heads == row // group, column // kv_heads, span)
    score_scale = head ** (-0.5)
    for load in loads[3:]:
        load.wait()

    def one_sequence(s, carry):
        owned = [table_ref[s, p] for p in range(pages)]
        length = lengths_ref[s]
        query = queries[s]
        cached = jnp.concatenate([keys[page] for page in owned], axis=0)
        scores = (
            lax.dot_general(
                query.astype(BF16),
                cached,
                (((1,), (1,)), ((), ())),
                preferred_element_type=F32,
            )
            * score_scale
        )
        new_score = jnp.sum(query * new_keys[s], axis=1, keepdims=True) * score_scale
        masked = jnp.where(place < length, scores, -jnp.inf)
        peak = jnp.maximum(jnp.max(masked, axis=1, keepdims=True), new_score)
        soft = jnp.exp(masked - peak)
        new_weight = jnp.exp(new_score - peak)
        denominator = jnp.sum(soft, axis=1, keepdims=True) + new_weight
        stored = jnp.concatenate([values[page] for page in owned], axis=0)
        result = jnp.dot(soft.astype(BF16), stored, preferred_element_type=F32)
        result = result + new_weight.astype(BF16).astype(F32) * new_values[s]
        mixed[s] = result / denominator
        return carry

    middle = seqs // 2
    lax.fori_loop(0, middle, one_sequence, 0, unroll=UNROLL)

    for copy in sum_copies:
        copy.wait_recv()
    row_sums = sums_all[0]
    for k in range(1, tp):
        row_sums = row_sums + sums_all[k]
    seq_row = lax.broadcasted_iota(jnp.int32, (seqs, sums_own.shape[1]), 0)
    counts = jnp.zeros(seq_row.shape, F32)
    for s in range(seqs):
        counts = jnp.where(seq_row == s, counts_ref[me * seqs + s].astype(F32), counts)
    residual = (row_sums - check_sum) / math.sqrt(total * tp)
    over = jnp.maximum(jnp.abs(residual) - TOL_STEP * counts, 0.0)
    excess_own[...] = jnp.broadcast_to(jnp.sum(over, axis=0, keepdims=True), excess_own.shape)
    excess_all[me] = excess_own[...]
    exc_copies = []
    for k in range(1, dp):
        copy = pltpu.make_async_remote_copy(
            src_ref=excess_own,
            dst_ref=excess_all.at[me],
            send_sem=exc_send.at[k],
            recv_sem=exc_recv.at[k],
            device_id=((me + k) % dp, zed),
            device_id_type=MESH,
        )
        copy.start()
        exc_copies.append(copy)

    lax.fori_loop(middle, seqs, one_sequence, 0, unroll=UNROLL)

    for h in range(q_heads):
        out_ref[:, h * head : (h + 1) * head] = mixed[:, h, :].astype(BF16)

    for copy in exc_copies:
        copy.wait_recv()
    grand = excess_all[0]
    for k in range(1, dp):
        grand = grand + excess_all[k]
    excess_ref[...] = grand / math.sqrt(seqs * dp)

    for copy in a2a + pair_copies + chip_copies + sum_copies + exc_copies:
        copy.wait_send()


def body(
    dp,
    tp,
    tokens,
    norm_gain,
    w_query,
    w_key,
    w_value,
    check_column,
    key_cache,
    value_cache,
    page_table,
    lengths,
    tol_counts,
):
    seqs, width = tokens.shape
    head = key_cache.shape[-1]
    q_width, kv_width = w_query.shape[1], w_key.shape[1]
    total = q_width + 2 * kv_width
    q_heads = q_width // head
    depth = width // dp
    chips = dp // 2
    chunks = 5 if total % (5 * head) == 0 else 1
    chunk = total // chunks
    half_width = head // 2
    steps_index = jnp.arange(half_width, dtype=F32)
    inverse = ROPE_BASE ** (-2.0 * steps_index / head)
    angles = lengths.astype(F32)[:, None] * inverse[None, :]
    cosine, sine = jnp.cos(angles), jnp.sin(angles)
    cos_wide = jnp.concatenate([cosine, cosine], axis=1)
    sin_wide = jnp.concatenate([-sine, sine], axis=1)
    flat_keys = key_cache.reshape(key_cache.shape[0], -1, head)
    flat_values = value_cache.reshape(value_cache.shape[0], -1, head)

    smem = pl.BlockSpec(memory_space=pltpu.SMEM)
    vmem = pl.BlockSpec(memory_space=pltpu.VMEM)
    hbm = pl.BlockSpec(memory_space=pl.ANY)
    dma = pltpu.SemaphoreType.DMA
    attention, excess = pl.pallas_call(
        functools.partial(step_kernel, dp, tp),
        out_shape=(
            jax.ShapeDtypeStruct((seqs, q_width), BF16),
            jax.ShapeDtypeStruct((8, 128), F32),
        ),
        in_specs=[smem] * 3 + [vmem] * 5 + [hbm] * 5,
        out_specs=(vmem, vmem),
        scratch_shapes=[
            pltpu.VMEM((depth, total), BF16),
            pltpu.VMEM(flat_keys.shape, BF16),
            pltpu.VMEM(flat_values.shape, BF16),
            pltpu.VMEM((dp, seqs, depth), BF16),
            pltpu.VMEM((2, chips, seqs, depth), BF16),
            pltpu.VMEM((chunks, 2, chips * seqs, chunk), F32),
            pltpu.VMEM((chunks, chips * seqs, chunk), F32),
            pltpu.VMEM((chunks, chips - 1, seqs, chunk), F32),
            pltpu.VMEM((seqs, q_heads, head), F32),
            pltpu.VMEM((seqs, q_heads, head), F32),
            pltpu.VMEM((seqs, q_heads, head), F32),
            pltpu.VMEM((seqs, q_heads, head), F32),
            pltpu.VMEM((tp, seqs, 128), F32),
            pltpu.VMEM((seqs, 128), F32),
            pltpu.VMEM((dp, 8, 128), F32),
            pltpu.VMEM((8, 128), F32),
            dma((5,)),
            dma((2, chips)),
            dma((2, chips)),
            dma((chunks,)),
            dma((chunks,)),
            dma((chunks, chips - 1)),
            dma((chunks, chips - 1)),
            dma((tp,)),
            dma((tp,)),
            dma((dp,)),
            dma((dp,)),
        ],
        compiler_params=pltpu.CompilerParams(
            collective_id=0, has_side_effects=True, vmem_limit_bytes=60 * 1024 * 1024
        ),
    )(
        page_table,
        lengths,
        tol_counts,
        tokens,
        norm_gain.reshape(1, width),
        check_column.reshape(1, width),
        cos_wide,
        sin_wide,
        w_query,
        w_key,
        w_value,
        flat_keys,
        flat_values,
    )
    return attention, excess[0, 0]


def solution(mesh):
    return jax.shard_map(
        functools.partial(body, mesh.shape["dp"], mesh.shape["tensor"]),
        mesh=mesh,
        in_specs=(
            P("dp", None),
            P(),
            P("dp", "tensor"),
            P("dp", "tensor"),
            P("dp", "tensor"),
            P(),
            P("dp", None, "tensor", None),
            P("dp", None, "tensor", None),
            P("dp", None),
            P("dp"),
            P(),
        ),
        out_specs=(P("dp", "tensor"), P()),
        check_vma=False,
    )
```

```python
import functools
import math

import jax
import jax.numpy as jnp
from jax import lax
from jax.experimental import pallas as pl
from jax.experimental.pallas import tpu as pltpu
from jax.sharding import PartitionSpec as P

EPSILON = 1e-06
ROPE_BASE = 1000000.0
TOL_STEP = 0.25
MESH = pl.DeviceIdType.MESH
F32 = jnp.float32
BF16 = jnp.bfloat16
UNROLL = 4
LANES = 128


def step_kernel(
    dp,
    tp,
    table_ref,
    lengths_ref,
    counts_ref,
    tokens_ref,
    gain_ref,
    check_ref,
    wq_hbm,
    wk_hbm,
    wv_hbm,
    keys_hbm,
    values_hbm,
    out_ref,
    excess_ref,
    weights,
    keys,
    values,
    outgoing,
    spread,
    parts,
    from_pair,
    from_chips,
    queries,
    new_keys,
    new_values,
    mixed,
    sums_all,
    sums_own,
    shares,
    excess_all,
    excess_own,
    load_sems,
    a2a_send,
    a2a_recv,
    pair_send,
    pair_recv,
    chip_send,
    chip_recv,
    sum_send,
    sum_recv,
    exc_send,
    exc_recv,
):
    chips = dp // 2
    me = lax.axis_index("dp")
    zed = lax.axis_index("tensor")
    chip, core = me // 2, me % 2
    seqs, width = tokens_ref.shape
    depth = width // dp
    q_width, kv_width = wq_hbm.shape[1], wk_hbm.shape[1]
    total = q_width + 2 * kv_width
    chunks, _, _, chunk = parts.shape
    head = keys_hbm.shape[2]
    q_heads, kv_heads = q_width // head, kv_width // head
    group = q_heads // kv_heads
    pages = table_ref.shape[1]
    page_rows = keys_hbm.shape[1]

    barrier = pltpu.get_barrier_semaphore()
    for k in range(1, dp):
        pl.semaphore_signal(
            barrier, inc=1, device_id=((me + k) % dp, zed), device_id_type=MESH
        )
    for k in range(1, tp):
        pl.semaphore_signal(
            barrier, inc=1, device_id=(me, (zed + k) % tp), device_id_type=MESH
        )

    loads = [
        pltpu.make_async_copy(wq_hbm, weights.at[:, pl.ds(0, q_width)], load_sems.at[0]),
        pltpu.make_async_copy(wk_hbm, weights.at[:, pl.ds(q_width, kv_width)], load_sems.at[1]),
        pltpu.make_async_copy(
            wv_hbm, weights.at[:, pl.ds(q_width + kv_width, kv_width)], load_sems.at[2]
        ),
        pltpu.make_async_copy(keys_hbm, keys, load_sems.at[3]),
        pltpu.make_async_copy(values_hbm, values, load_sems.at[4]),
    ]
    for load in loads:
        load.start()

    square = jnp.zeros((seqs, LANES), F32)
    for j in range(width // LANES):
        part = tokens_ref[:, j * LANES : (j + 1) * LANES].astype(F32)
        square = square + part * part
    scale = lax.rsqrt(jnp.sum(square, axis=1, keepdims=True) / width + EPSILON)
    gains = gain_ref[...].astype(F32)
    for j in range(width // LANES):
        part = tokens_ref[:, j * LANES : (j + 1) * LANES].astype(F32)
        at = j * LANES % depth
        outgoing[j * LANES // depth, :, at : at + LANES] = (
            part * scale * gains[j : j + 1]
        ).astype(BF16)
    spread[0, 0] = outgoing[me]

    pl.semaphore_wait(barrier, dp - 1 + tp - 1)

    a2a = []
    for dc in range(chips - 1, -1, -1):
        for q in range(2):
            if dc == 0 and q == 0:
                continue
            target = ((chip + dc) % chips) * 2 + (core + q) % 2
            copy = pltpu.make_async_remote_copy(
                src_ref=outgoing.at[target],
                dst_ref=spread.at[q, dc],
                send_sem=a2a_send.at[q, dc],
                recv_sem=a2a_recv.at[q, dc],
                device_id=(target, zed),
                device_id_type=MESH,
            )
            copy.start()
            a2a.append(copy)

    checks = check_ref[...].astype(F32)
    checked = jnp.zeros((seqs, LANES), F32)
    for j in range(width // LANES):
        at = j * LANES % depth
        part = outgoing[j * LANES // depth, :, at : at + LANES].astype(F32)
        checked = checked + part * checks[j : j + 1]

    seq_row = lax.broadcasted_iota(jnp.int32, (seqs, LANES), 0)
    positions = jnp.zeros((seqs, LANES), F32)
    for s in range(seqs):
        positions = jnp.where(seq_row == s, lengths_ref[s].astype(F32), positions)
    lane = lax.broadcasted_iota(jnp.int32, (seqs, head), 1)
    step = (lane % (head // 2)).astype(F32)
    angles = positions * jnp.exp(step * (-2.0 * math.log(ROPE_BASE) / head))
    cosine = jnp.cos(angles)
    sine = jnp.where(lane < head // 2, -1.0, 1.0) * jnp.sin(angles)

    for load in loads[:3]:
        load.wait()
    for copy in a2a:
        copy.wait_recv()

    pair_copies, chip_copies = [], []
    half = chips * seqs

    def project(c):
        product = jnp.dot(
            spread[...].reshape(dp * seqs, depth),
            weights[:, pl.ds(c * chunk, chunk)],
            preferred_element_type=F32,
        )
        parts[c, 1] = product[half:]
        copy = pltpu.make_async_remote_copy(
            src_ref=parts.at[c, 1],
            dst_ref=from_pair.at[c],
            send_sem=pair_send.at[c],
            recv_sem=pair_recv.at[c],
            device_id=(chip * 2 + (core + 1) % 2, zed),
            device_id_type=MESH,
        )
        copy.start()
        pair_copies.append(copy)
        parts[c, 0] = product[:half]
        return sum(product[:, i : i + LANES] for i in range(0, chunk, LANES))

    def pass_on(c):
        pair_copies[c].wait_recv()
        for dc in range(chips - 1, 0, -1):
            rows = pl.ds(dc * seqs, seqs)
            parts[c, 0, rows] = parts[c, 0, rows] + from_pair[c, rows]
            copy = pltpu.make_async_remote_copy(
                src_ref=parts.at[c, 0, rows],
                dst_ref=from_chips.at[c, dc - 1],
                send_sem=chip_send.at[c, dc - 1],
                recv_sem=chip_recv.at[c, dc - 1],
                device_id=(((chip + chips - dc) % chips) * 2 + core, zed),
                device_id_type=MESH,
            )
            copy.start()
            chip_copies.append(copy)

    def exchange(own, everyone, place, targets, send_sems, recv_sems):
        everyone[place] = own[...]
        copies = []
        for k, target in enumerate(targets):
            copy = pltpu.make_async_remote_copy(
                src_ref=own,
                dst_ref=everyone.at[place],
                send_sem=send_sems.at[k],
                recv_sem=recv_sems.at[k],
                device_id=target,
                device_id_type=MESH,
            )
            copy.start()
            copies.append(copy)
        return copies

    row_sum = jnp.zeros((dp * seqs, LANES), F32)
    for c in range(chunks):
        row_sum = row_sum + project(c)
        if c >= 1:
            pass_on(c - 1)
    for q in range(2):
        for dc in range(chips):
            owner = ((chip + chips - dc) % chips) * 2 + (core + q) % 2
            at = (q * chips + dc) * seqs
            share = row_sum[at : at + seqs]
            if q == 0 and dc == 0:
                share = share - jnp.where(zed == 0, checked, 0.0)
            shares[owner] = share
    turned_sums = jnp.transpose(shares[...].reshape(dp * seqs, LANES))
    excess_own[...] = jnp.sum(turned_sums, axis=0, keepdims=True)
    exc_copies = exchange(
        excess_own, excess_all, me, [((me + k) % dp, zed) for k in range(1, dp)], exc_send, exc_recv
    )
    pass_on(chunks - 1)
    for copy in exc_copies:
        copy.wait_recv()
    group_sum = excess_all[0]
    for k in range(1, dp):
        group_sum = group_sum + excess_all[k]
    sums_own[...] = group_sum
    sum_copies = exchange(
        sums_own, sums_all, zed, [(me, (zed + k) % tp) for k in range(1, tp)], sum_send, sum_recv
    )

    def rotate(vector):
        return (
            (vector * cosine + pltpu.roll(vector, head // 2, 1) * sine)
            .astype(BF16)
            .astype(F32)
        )

    for c in range(chunks):
        for copy in chip_copies[c * (chips - 1) : (c + 1) * (chips - 1)]:
            copy.wait_recv()
        own = parts[c, 0, pl.ds(0, seqs)] + from_pair[c, pl.ds(0, seqs)]
        for dc in range(1, chips):
            own = own + from_chips[c, dc - 1]
        for i in range(chunk // head):
            block = own[:, i * head : (i + 1) * head]
            index = c * (chunk // head) + i
            if index < q_heads:
                queries[:, index, :] = rotate(block)
            elif index < q_heads + kv_heads:
                k = index - q_heads
                turned = rotate(block)
                for g in range(group):
                    new_keys[:, k * group + g, :] = turned
            else:
                k = index - q_heads - kv_heads
                rounded = block.astype(BF16).astype(F32)
                for g in range(group):
                    new_values[:, k * group + g, :] = rounded

    span = pages * page_rows
    column = lax.broadcasted_iota(jnp.int32, (q_heads, span), 1)
    row = lax.broadcasted_iota(jnp.int32, (q_heads, span), 0)
    place = jnp.where(column % kv_heads == row // group, column // kv_heads, span)
    score_scale = head ** (-0.5)
    for load in loads[3:]:
        load.wait()

    def one_sequence(s, carry):
        owned = [table_ref[s, p] for p in range(pages)]
        length = lengths_ref[s]
        query = queries[s]
        cached = jnp.concatenate([keys[page] for page in owned], axis=0)
        scores = (
            lax.dot_general(
                query.astype(BF16),
                cached,
                (((1,), (1,)), ((), ())),
                preferred_element_type=F32,
            )
            * score_scale
        )
        new_score = jnp.sum(query * new_keys[s], axis=1, keepdims=True) * score_scale
        masked = jnp.where(place < length, scores, -jnp.inf)
        peak = jnp.maximum(jnp.max(masked, axis=1, keepdims=True), new_score)
        soft = jnp.exp(masked - peak)
        new_weight = jnp.exp(new_score - peak)
        denominator = jnp.sum(soft, axis=1, keepdims=True) + new_weight
        stored = jnp.concatenate([values[page] for page in owned], axis=0)
        result = jnp.dot(soft.astype(BF16), stored, preferred_element_type=F32)
        result = result + new_weight.astype(BF16).astype(F32) * new_values[s]
        mixed[s] = result / denominator
        return carry

    lax.fori_loop(0, seqs, one_sequence, 0, unroll=UNROLL)

    for h in range(q_heads):
        out_ref[:, h * head : (h + 1) * head] = mixed[:, h, :].astype(BF16)

    for copy in sum_copies:
        copy.wait_recv()
    grand = sums_all[0]
    for k in range(1, tp):
        grand = grand + sums_all[k]
    residual = grand / math.sqrt(total * tp)
    over = jnp.maximum(jnp.abs(residual) - TOL_STEP * counts_ref[...].astype(F32), 0.0)
    excess_ref[...] = jnp.sum(over, axis=1, keepdims=True) / math.sqrt(seqs * dp)

    for copy in a2a + pair_copies + chip_copies + sum_copies + exc_copies:
        copy.wait_send()


def body(
    dp,
    tp,
    tokens,
    norm_gain,
    w_query,
    w_key,
    w_value,
    check_column,
    key_cache,
    value_cache,
    page_table,
    lengths,
    tol_counts,
):
    seqs, width = tokens.shape
    head = key_cache.shape[-1]
    q_width, kv_width = w_query.shape[1], w_key.shape[1]
    total = q_width + 2 * kv_width
    q_heads = q_width // head
    depth = width // dp
    chips = dp // 2
    chunks = 5 if total % (5 * head) == 0 else 1
    chunk = total // chunks
    flat_keys = key_cache.reshape(key_cache.shape[0], -1, head)
    flat_values = value_cache.reshape(value_cache.shape[0], -1, head)

    smem = pl.BlockSpec(memory_space=pltpu.SMEM)
    vmem = pl.BlockSpec(memory_space=pltpu.VMEM)
    hbm = pl.BlockSpec(memory_space=pltpu.HBM)
    dma = pltpu.SemaphoreType.DMA
    attention, excess = pl.pallas_call(
        functools.partial(step_kernel, dp, tp),
        out_shape=(
            jax.ShapeDtypeStruct((seqs, q_width), BF16),
            jax.ShapeDtypeStruct((1, 1), F32),
        ),
        in_specs=[smem] * 2 + [vmem] * 4 + [hbm] * 5,
        out_specs=(vmem, vmem),
        scratch_shapes=[
            pltpu.VMEM((depth, total), BF16),
            pltpu.VMEM(flat_keys.shape, BF16),
            pltpu.VMEM(flat_values.shape, BF16),
            pltpu.VMEM((dp, seqs, depth), BF16),
            pltpu.VMEM((2, chips, seqs, depth), BF16),
            pltpu.VMEM((chunks, 2, chips * seqs, chunk), F32),
            pltpu.VMEM((chunks, chips * seqs, chunk), F32),
            pltpu.VMEM((chunks, chips - 1, seqs, chunk), F32),
            pltpu.VMEM((seqs, q_heads, head), F32),
            pltpu.VMEM((seqs, q_heads, head), F32),
            pltpu.VMEM((seqs, q_heads, head), F32),
            pltpu.VMEM((seqs, q_heads, head), F32),
            pltpu.VMEM((tp, 1, dp * seqs), F32),
            pltpu.VMEM((1, dp * seqs), F32),
            pltpu.VMEM((dp, seqs, LANES), F32),
            pltpu.VMEM((dp, 1, dp * seqs), F32),
            pltpu.VMEM((1, dp * seqs), F32),
            dma((5,)),
            dma((2, chips)),
            dma((2, chips)),
            dma((chunks,)),
            dma((chunks,)),
            dma((chunks, chips - 1)),
            dma((chunks, chips - 1)),
            dma((tp,)),
            dma((tp,)),
            dma((dp,)),
            dma((dp,)),
        ],
        compiler_params=pltpu.CompilerParams(
            collective_id=0, has_side_effects=True, vmem_limit_bytes=60 * 1024 * 1024
        ),
    )(
        page_table,
        lengths,
        tol_counts.reshape(1, -1),
        tokens,
        norm_gain.reshape(-1, LANES),
        check_column.reshape(-1, LANES),
        w_query,
        w_key,
        w_value,
        flat_keys,
        flat_values,
    )
    return attention, excess[0, 0]


def solution(mesh):
    return jax.shard_map(
        functools.partial(body, mesh.shape["dp"], mesh.shape["tensor"]),
        mesh=mesh,
        in_specs=(
            P("dp", None),
            P(),
            P("dp", "tensor"),
            P("dp", "tensor"),
            P("dp", "tensor"),
            P(),
            P("dp", None, "tensor", None),
            P("dp", None, "tensor", None),
            P("dp", None),
            P("dp"),
            P(),
        ),
        out_specs=(P("dp", "tensor"), P()),
        check_vma=False,
    )
```
